256 devices in a mesh: trial: 2 (over core), qa: 16 (over y, x), qb: 8 (over z).
Axes of the slice: x: 4, y: 4, z: 8, core: 2. Of those that a mesh axis runs over, the one named last changes fastest.
Arguments:
- wave_parts: float32 [4, 512, 128, 128], P('trial', ('qa', 'qb')), parts along dimension 0, may hold values from -6 to 6
- level_table: float32 [1024, 128, 128], P(('trial', 'qa', 'qb')), parts along dimension 0, may hold values from -2 to 2
- diagonal_angles: float32 [6, 128], P('trial'), parts along dimension 0, may hold values from 0.3 to 1.2
- turn_angles: float32 [6, 4], P('trial'), parts along dimension 0, may hold values from 0.3 to 1.2
Outputs:
- final_parts: float32 [4, 512, 128, 128], P('trial', ('qa', 'qb')), parts along dimension 0
The draws below stay inside these ranges and needn't reach their ends.
There are 2 independent parts, one for each index of `trial`. The reference program is written for one: setup_inputs(seed, part) draws one part's arguments, and reference() takes and returns one part's arrays. A program takes and returns all parts, laid end to end along the dimension named above; each array names one. Nothing has to cross between parts.
All inputs are finite; a program needn't handle non-finite values.
Results may differ from the reference program's by a relative error of at most 0.0003.
Values sent between devices are 32-bit elements.
A program may use at most 64 MiB of HBM per device.

```python
import jax
import jax.numpy as jnp
from jax import lax

BLOCKS_DEV = 4
ROWS = 128
LANES = 128
BLOCKS = 512
LAYERS = 3
N_QA = 16
N_QB = 8


def block_scale(own_key, dims, pieces, smallest, high):
    def one(position, blocks):
        heights = jax.random.uniform(jax.random.fold_in(jax.random.fold_in(own_key, 6), position), (blocks,), jnp.float32, smallest / len(pieces), high / len(pieces))
        return jnp.repeat(jnp.exp(heights), dims[position] // blocks).reshape((-1,) + (1,) * (len(dims) - position - 1))

    factor_of = one(*pieces[0])
    for cut in pieces[1:]:
        factor_of = factor_of * one(*cut)
    return factor_of


def scatter_about(rng, dims, spread, most, cuts=(), kind=jnp.bfloat16):
    values = spread * jax.random.normal(rng, dims, jnp.float32)
    if cuts:
        values = values * block_scale(rng, dims, cuts, -0.22, 0.18)
    return jnp.clip(values, -most, most).astype(kind)


def setup_inputs(seed: int = 0, part: int = 0) -> dict:
    key_of = jax.random.split(jax.random.key(seed), 5)
    own_keys = jax.random.split(jax.random.fold_in(key_of[4], part), 5)
    wave_parts = scatter_about(own_keys[0], (2, BLOCKS, ROWS, LANES), 1.0, 6.0, ((1, 128),), jnp.float32)
    level_table = jnp.clip(jax.random.uniform(own_keys[1], (BLOCKS, ROWS, LANES), jnp.float32, -2.0, 2.0) * block_scale(own_keys[1], (BLOCKS, ROWS, LANES), ((0, 128),), -0.4, 0.0), -2.0, 2.0)
    diagonal_angles = jnp.clip(jax.random.uniform(own_keys[2], (LAYERS, LANES), jnp.float32, 0.3, 1.2), 0.3, 1.2)
    turn_angles = jnp.clip(jax.random.uniform(own_keys[3], (LAYERS, 4), jnp.float32, 0.3, 1.2), 0.3, 1.2)
    return dict(wave_parts=wave_parts, level_table=level_table, diagonal_angles=diagonal_angles, turn_angles=turn_angles)


def count_bits(values, count):
    places = jnp.arange(count.bit_length() - 1, dtype=jnp.int32)
    return jnp.sum((values[..., None] >> places) & 1, axis=-1)


def rotation_table(count, angle):
    rank = jnp.arange(count, dtype=jnp.int32)
    apart = count_bits(rank[:, None] ^ rank[None, :], count)
    bits = count.bit_length() - 1
    size = jnp.cos(angle) ** (bits - apart).astype(jnp.float32) * jnp.sin(angle) ** apart.astype(jnp.float32)
    real_sign = jnp.where(apart % 4 == 0, 1.0, jnp.where(apart % 4 == 2, -1.0, 0.0)).astype(jnp.float32)
    imag_sign = jnp.where(apart % 4 == 1, -1.0, jnp.where(apart % 4 == 3, 1.0, 0.0)).astype(jnp.float32)
    return size * real_sign, size * imag_sign


def mix_dim(values, dim, angle):
    real_part, imag_part = rotation_table(values.shape[dim], angle)
    def times(table):
        moved = jnp.tensordot(values, table, axes=([dim], [0]), precision=lax.Precision.HIGHEST)
        return jnp.moveaxis(moved, -1, dim)
    by_real = times(real_part)
    by_imag = times(imag_part)
    return jnp.stack([by_real[0] - by_imag[1], by_real[1] + by_imag[0]])


def phase_step(values, levels, angle):
    turn = angle * levels
    return jnp.stack([values[0] * jnp.cos(turn) + values[1] * jnp.sin(turn), values[1] * jnp.cos(turn) - values[0] * jnp.sin(turn)])


def reference(wave_parts, level_table, diagonal_angles, turn_angles):
    values = wave_parts
    for layer in range(LAYERS):
        values = phase_step(values, level_table, diagonal_angles[layer])
        values = mix_dim(values, 3, turn_angles[layer, 0])
        values = mix_dim(values, 2, turn_angles[layer, 1])
        parts = values.reshape(2, N_QA, N_QB, BLOCKS_DEV, ROWS, LANES)
        parts = mix_dim(parts, 1, turn_angles[layer, 2])
        parts = mix_dim(parts, 2, turn_angles[layer, 3])
        parts = mix_dim(parts, 3, turn_angles[layer, 2])
        values = parts.reshape(values.shape)
    return values
```

```python
import functools

import jax
import jax.numpy as jnp
from jax import lax
from jax.experimental import pallas as pl
from jax.experimental.pallas import tpu as pltpu
from jax.sharding import PartitionSpec as P

MESH = pl.DeviceIdType.MESH
F32 = jnp.float32
BF16 = jnp.bfloat16
PAD = 8


def split(x):
    high = x.astype(BF16)
    return high, (x - high.astype(F32)).astype(BF16)


def dot3(a, b, dims=((1,), (0,))):
    def one(x, y):
        return lax.dot_general(x, y, (dims, ((), ())), preferred_element_type=F32)

    (ah, al), (bh, bl) = a, b
    return one(ah, bh) + (one(ah, bl) + one(al, bh))


def sincos(x):
    turns = jnp.floor(x * 0.6366197723675814 + 0.5)
    y = (x - turns * 1.5707855224609375) - turns * 1.0804334124e-05
    z = y * y
    s = y + y * z * (-1.6666654611e-1 + z * (8.3321608736e-3 + z * -1.9515295891e-4))
    c = 1.0 - 0.5 * z + z * z * (4.166664568298827e-2 + z * (-1.388731625493765e-3 + z * 2.443315711809948e-5))
    quarter = turns - 4.0 * jnp.floor(turns * 0.25)
    odd = (quarter == 1.0) | (quarter == 3.0)
    sin = jnp.where(odd, c, s)
    cos = jnp.where(odd, s, c)
    sin = jnp.where(quarter >= 2.0, -sin, sin)
    cos = jnp.where((quarter == 1.0) | (quarter == 2.0), -cos, cos)
    return sin, cos


def phased(xr, xi, turn):
    s, c = sincos(turn)
    return xr * c + xi * s, xi * c - xr * s


def rotation(count, pairs):
    apart = lax.broadcasted_iota(jnp.int32, (count, count), 0) ^ lax.broadcasted_iota(jnp.int32, (count, count), 1)
    size = None
    ones = None
    for place, (c, s) in enumerate(pairs):
        bit = (apart >> place) & 1
        factor = jnp.where(bit == 1, s, c)
        size = factor if size is None else size * factor
        ones = bit if ones is None else ones + bit
    ones = ones & 3
    real = jnp.where(ones == 0, size, jnp.where(ones == 2, -size, 0.0))
    imag = jnp.where(ones == 1, -size, jnp.where(ones == 3, size, 0.0))
    return real, imag


def mix_blocks(parts, c, s):
    step = 1
    while step < len(parts):
        mixed = list(parts)
        for k in range(len(parts)):
            if not k & step:
                (ur, ui), (vr, vi) = parts[k], parts[k | step]
                mixed[k] = (c * ur + s * vi, c * ui - s * vr)
                mixed[k | step] = (c * vr + s * ui, c * vi - s * ur)
        parts = mixed
        step *= 2
    return parts


def body(
    nqa,
    nqb,
    wave,
    levels,
    diag,
    turns,
    out,
    mats,
    send1,
    send2,
    send3,
    land1,
    land2,
    land3,
    flip,
    tab2,
    tab3,
    work,
    ssem,
    rsem,
    tsend,
    trecv,
):
    n = nqa * nqb
    blocks = wave.shape[1]
    qa = lax.axis_index("qa")
    qb = lax.axis_index("qb")
    me = qa * nqb + qb
    near = list(range(1, nqb))
    near.sort(key=lambda d: -min(d, nqb - d))

    def peers(visit):
        @pl.loop(1, nqa)
        def _(da):
            for dz in near + [0]:
                visit(lax.rem(qa + da, nqa), lax.rem(qb + dz, nqb))

        for dz in near:
            visit(qa, lax.rem(qb + dz, nqb))

    bar = pltpu.get_barrier_semaphore()
    peers(lambda a, z: pl.semaphore_signal(bar, inc=1, device_id={"qa": a, "qb": z}, device_id_type=MESH))

    def spread(src, dst, ssem, rsem):
        def visit(a, z):
            pltpu.make_async_remote_copy(
                src_ref=src.at[:, pl.ds(a * nqb + z, 1), :],
                dst_ref=dst.at[:, pl.ds(me, 1), :],
                send_sem=ssem,
                recv_sem=rsem,
                device_id={"qa": a, "qb": z},
                device_id_type=MESH,
            ).start()

        peers(visit)
        pltpu.make_async_remote_copy(
            src_ref=src.at[:, pl.ds(0, 1), :],
            dst_ref=dst.at[:, pl.ds(n, 1), :],
            send_sem=ssem,
            recv_sem=rsem,
            device_id={"qa": qa, "qb": lax.rem(qb + 1, nqb)},
            device_id_type=MESH,
        ).start()
        dst[:, pl.ds(me, 1), :] = src[:, pl.ds(me, 1), :]

    def landed(dst, rsem):
        whole = dst.at[:, pl.ds(0, n), :]
        pltpu.make_async_copy(whole, whole, rsem).wait()

    turn_sin, turn_cos = sincos(turns[...])

    def pair(layer, group):
        return turn_cos[layer : layer + 1, group : group + 1], turn_sin[layer : layer + 1, group : group + 1]

    bits = n.bit_length() - 1
    low = nqb.bit_length() - 1

    def build(slot, layer, groups, left):
        real, imag = rotation(n, [pair(layer, g) for g in groups])
        if left:
            whole = jnp.concatenate(
                [jnp.concatenate([real, -imag], axis=1), jnp.concatenate([imag, real], axis=1)], axis=0
            )
        else:
            whole = jnp.concatenate(
                [jnp.concatenate([real, imag], axis=1), jnp.concatenate([-imag, real], axis=1)], axis=0
            )
        high, rest = split(whole)
        mats[slot, 0] = high
        mats[slot, 1] = rest

    device_groups = [3] * low + [2] * (bits - low)
    LANE1, ROW1, DEV1, LANE2, ROW2, DEV2, DEV3, ROW3, LANE3 = range(9)

    def mat(slot):
        return mats[slot, 0], mats[slot, 1]

    def left(slot, xr, xi):
        both = dot3(mat(slot), split(jnp.concatenate([xr, xi], axis=0)))
        return both[:n], both[n:]

    def right(slot, xr, xi):
        both = dot3(split(jnp.concatenate([xr, xi], axis=1)), mat(slot))
        return both[:, :n], both[:, n:]

    def turned(slot, xr, xi):
        both = dot3(mat(slot), split(jnp.concatenate([xr, xi], axis=1)), ((1,), (1,)))
        return both[:n], both[n:]

    for b in range(blocks):
        flip[b] = levels[b].T
    pl.semaphore_wait(bar, n - 1)
    spread(levels, tab2, tsend.at[0], trecv.at[0])

    build(LANE1, 0, [0] * bits, False)
    build(ROW1, 0, [1] * bits, True)
    parts = [phased(wave[0, b], wave[1, b], diag[0:1, :] * levels[b]) for b in range(blocks)]
    parts = mix_blocks(parts, *pair(0, 2))
    for b in range(blocks):
        work[b, 0], work[b, 1] = parts[b]

    @pl.loop(0, blocks)
    def _(b):
        xr, xi = right(LANE1, work[b, 0], work[b, 1])
        send1[b, 0], send1[b, 1] = left(ROW1, xr, xi)
        spread(send1.at[b], land1.at[b], ssem.at[b], rsem.at[b])

    build(DEV1, 0, device_groups, True)
    build(LANE2, 1, [0] * bits, True)
    build(ROW2, 1, [1] * bits, True)
    build(DEV2, 1, device_groups, True)
    build(DEV3, 2, device_groups, True)
    build(ROW3, 2, [1] * bits, False)
    build(LANE3, 2, [0] * bits, False)

    landed(tab2, trecv.at[0])

    @pl.loop(0, blocks)
    def _(b):
        landed(land1.at[b], rsem.at[b])
        xr, xi = left(DEV1, land1[b, 0, :n, :], land1[b, 1, :n, :])
        xr, xi = phased(xr, xi, diag[1:2, :] * tab2[b, :n, :])
        send2[b, 0], send2[b, 1] = turned(LANE2, xr, xi)
        spread(send2.at[b], land2.at[b], ssem.at[blocks + b], rsem.at[blocks + b])

    spread(flip, tab3, tsend.at[1], trecv.at[1])

    @pl.loop(0, blocks)
    def _(b):
        landed(land2.at[b], rsem.at[blocks + b])
        xr, xi = left(ROW2, land2[b, 0, :n, :], land2[b, 1, :n, :])
        work[b, 0], work[b, 1] = turned(DEV2, xr, xi)

    parts = mix_blocks([(work[b, 0], work[b, 1]) for b in range(blocks)], *pair(1, 2))
    for b in range(blocks):
        work[b, 0], work[b, 1] = parts[b]
    landed(tab3, trecv.at[1])
    lane = lax.broadcasted_iota(jnp.int32, (1, n), 1)
    own = jnp.sum(jnp.where(lane == me, diag[2:3, :], 0.0), axis=1, keepdims=True)

    @pl.loop(0, blocks)
    def _(b):
        xr, xi = phased(work[b, 0], work[b, 1], own * tab3[b, :n, :])
        xr, xi = left(DEV3, xr, xi)
        send3[b, 0], send3[b, 1] = right(ROW3, xr, xi)
        spread(send3.at[b], land3.at[b], ssem.at[2 * blocks + b], rsem.at[2 * blocks + b])

    @pl.loop(0, blocks)
    def _(b):
        landed(land3.at[b], rsem.at[2 * blocks + b])
        work[b, 0], work[b, 1] = right(LANE3, land3[b, 0, :n, :].T, land3[b, 1, :n, :].T)

    parts = mix_blocks([(work[b, 0], work[b, 1]) for b in range(blocks)], *pair(2, 2))
    for b in range(blocks):
        out[0, b], out[1, b] = parts[b]

    @pl.loop(0, blocks)
    def _(b):
        for k, (src, dst) in enumerate(((send1, land1), (send2, land2), (send3, land3))):
            landed(dst.at[b], ssem.at[k * blocks + b])

    landed(tab2, tsend.at[0])
    landed(tab3, tsend.at[1])


def solution(mesh):
    nqa, nqb = mesh.shape["qa"], mesh.shape["qb"]

    def shards(wave_parts, level_table, diagonal_angles, turn_angles):
        _, blocks, rows, lanes = wave_parts.shape
        state = pltpu.VMEM((blocks, 2, rows, lanes), F32)
        landing = pltpu.VMEM((blocks, 2, rows + PAD, lanes), F32)
        vmem = pl.BlockSpec(memory_space=pltpu.VMEM)
        return pl.pallas_call(
            functools.partial(body, nqa, nqb),
            out_shape=jax.ShapeDtypeStruct(wave_parts.shape, F32),
            in_specs=[vmem] * 4,
            out_specs=vmem,
            scratch_shapes=[
                pltpu.VMEM((9, 2, 2 * rows, 2 * lanes), BF16),
                state,
                state,
                state,
                landing,
                landing,
                landing,
                pltpu.VMEM((blocks, rows, lanes), F32),
                pltpu.VMEM((blocks, rows + PAD, lanes), F32),
                pltpu.VMEM((blocks, rows + PAD, lanes), F32),
                state,
                pltpu.SemaphoreType.DMA((3 * blocks,)),
                pltpu.SemaphoreType.DMA((3 * blocks,)),
                pltpu.SemaphoreType.DMA((2,)),
                pltpu.SemaphoreType.DMA((2,)),
            ],
            name="layers",
            compiler_params=pltpu.CompilerParams(collective_id=0, has_side_effects=True),
        )(wave_parts, level_table, diagonal_angles, turn_angles)

    return jax.shard_map(
        shards,
        mesh=mesh,
        in_specs=(
            P("trial", ("qa", "qb"), None, None),
            P(("trial", "qa", "qb"), None, None),
            P("trial", None),
            P("trial", None),
        ),
        out_specs=P("trial", ("qa", "qb"), None, None),
        check_vma=False,
    )
```

```python
import functools

import jax
import jax.numpy as jnp
from jax import lax
from jax.experimental import pallas as pl
from jax.experimental.pallas import tpu as pltpu
from jax.sharding import PartitionSpec as P

MESH = pl.DeviceIdType.MESH
F32 = jnp.float32
BF16 = jnp.bfloat16
PAD = 8
GROUP = 4
EARLY = True


def split(x):
    high = x.astype(BF16)
    return high, (x - high.astype(F32)).astype(BF16)


def dot3(a, b, dims=((1,), (0,))):
    def one(x, y):
        return lax.dot_general(x, y, (dims, ((), ())), preferred_element_type=F32)

    (ah, al), (bh, bl) = a, b
    return one(ah, bh) + (one(ah, bl) + one(al, bh))


def sincos(x):
    turns = jnp.floor(x * 0.6366197723675814 + 0.5)
    y = (x - turns * 1.5707855224609375) - turns * 1.0804334124e-05
    z = y * y
    s = y + y * z * (-1.6666654611e-1 + z * (8.3321608736e-3 + z * -1.9515295891e-4))
    c = 1.0 - 0.5 * z + z * z * (4.166664568298827e-2 + z * (-1.388731625493765e-3 + z * 2.443315711809948e-5))
    quarter = turns - 4.0 * jnp.floor(turns * 0.25)
    odd = (quarter == 1.0) | (quarter == 3.0)
    sin = jnp.where(odd, c, s)
    cos = jnp.where(odd, s, c)
    sin = jnp.where(quarter >= 2.0, -sin, sin)
    cos = jnp.where((quarter == 1.0) | (quarter == 2.0), -cos, cos)
    return sin, cos


def phased(xr, xi, turn):
    s, c = sincos(turn)
    return xr * c + xi * s, xi * c - xr * s


def rotation(count, pairs):
    apart = lax.broadcasted_iota(jnp.int32, (count, count), 0) ^ lax.broadcasted_iota(jnp.int32, (count, count), 1)
    size = None
    ones = None
    for place, (c, s) in enumerate(pairs):
        bit = (apart >> place) & 1
        factor = jnp.where(bit == 1, s, c)
        size = factor if size is None else size * factor
        ones = bit if ones is None else ones + bit
    ones = ones & 3
    real = jnp.where(ones == 0, size, jnp.where(ones == 2, -size, 0.0))
    imag = jnp.where(ones == 1, -size, jnp.where(ones == 3, size, 0.0))
    return real, imag


def mix_blocks(parts, c, s):
    step = 1
    while step < len(parts):
        mixed = list(parts)
        for k in range(len(parts)):
            if not k & step:
                (ur, ui), (vr, vi) = parts[k], parts[k | step]
                mixed[k] = (c * ur + s * vi, c * ui - s * vr)
                mixed[k | step] = (c * vr + s * ui, c * vi - s * ur)
        parts = mixed
        step *= 2
    return parts


def body(
    nqa,
    nqb,
    wave,
    levels,
    diag,
    turns,
    out,
    mats,
    send1,
    send2,
    send3,
    land1,
    land2,
    land3,
    flip,
    tab2,
    tab3,
    work,
    ssem,
    rsem,
    tsend,
    trecv,
):
    n = nqa * nqb
    blocks = wave.shape[1]
    qa = lax.axis_index("qa")
    qb = lax.axis_index("qb")
    me = qa * nqb + qb
    near = list(range(1, nqb))
    near.sort(key=lambda d: -min(d, nqb - d))

    def peers(visit):
        @pl.loop(1, nqa)
        def _(da):
            for dz in near + [0]:
                visit(lax.rem(qa + da, nqa), lax.rem(qb + dz, nqb))

        for dz in near:
            visit(qa, lax.rem(qb + dz, nqb))

    bar = pltpu.get_barrier_semaphore()
    peers(lambda a, z: pl.semaphore_signal(bar, inc=1, device_id={"qa": a, "qb": z}, device_id_type=MESH))

    def spread(src, dst, ssem, rsem):
        def visit(a, z):
            pltpu.make_async_remote_copy(
                src_ref=src.at[..., pl.ds(a * nqb + z, 1), :],
                dst_ref=dst.at[..., pl.ds(me, 1), :],
                send_sem=ssem,
                recv_sem=rsem,
                device_id={"qa": a, "qb": z},
                device_id_type=MESH,
            ).start()

        peers(visit)
        pltpu.make_async_remote_copy(
            src_ref=src.at[..., pl.ds(0, 1), :],
            dst_ref=dst.at[..., pl.ds(n, 1), :],
            send_sem=ssem,
            recv_sem=rsem,
            device_id={"qa": qa, "qb": lax.rem(qb + 1, nqb)},
            device_id_type=MESH,
        ).start()
        dst[..., pl.ds(me, 1), :] = src[..., pl.ds(me, 1), :]

    def swap(k, i):
        part = pl.ds(i * GROUP, GROUP)
        spread((send1, send2, send3)[k].at[part], (land1, land2, land3)[k].at[part], ssem.at[k, i], rsem.at[k, i])

    def arrived(k, i, sems):
        landed((land1, land2, land3)[k].at[pl.ds(i * GROUP, GROUP)], sems.at[k, i])

    def landed(dst, rsem):
        whole = dst.at[..., pl.ds(0, n), :]
        pltpu.make_async_copy(whole, whole, rsem).wait()

    turn_sin, turn_cos = sincos(turns[...])

    def pair(layer, group):
        return turn_cos[layer : layer + 1, group : group + 1], turn_sin[layer : layer + 1, group : group + 1]

    bits = n.bit_length() - 1
    low = nqb.bit_length() - 1

    def build(slot, layer, groups, left):
        real, imag = rotation(n, [pair(layer, g) for g in groups])
        if left:
            whole = jnp.concatenate(
                [jnp.concatenate([real, -imag], axis=1), jnp.concatenate([imag, real], axis=1)], axis=0
            )
        else:
            whole = jnp.concatenate(
                [jnp.concatenate([real, imag], axis=1), jnp.concatenate([-imag, real], axis=1)], axis=0
            )
        high, rest = split(whole)
        mats[slot, 0] = high
        mats[slot, 1] = rest

    device_groups = [3] * low + [2] * (bits - low)
    LANE1, ROW1, DEV1, LANE2, ROW2, DEV2, DEV3, ROW3, LANE3 = range(9)

    def mat(slot):
        return mats[slot, 0], mats[slot, 1]

    def left(slot, xr, xi):
        both = dot3(mat(slot), split(jnp.concatenate([xr, xi], axis=0)))
        return both[:n], both[n:]

    def right(slot, xr, xi):
        both = dot3(split(jnp.concatenate([xr, xi], axis=1)), mat(slot))
        return both[:, :n], both[:, n:]

    def turned(slot, xr, xi):
        both = dot3(mat(slot), split(jnp.concatenate([xr, xi], axis=1)), ((1,), (1,)))
        return both[:n], both[n:]

    for b in range(blocks):
        flip[b] = levels[b].T
    pl.semaphore_wait(bar, n - 1)
    spread(levels, tab2, tsend.at[0], trecv.at[0])

    build(LANE1, 0, [0] * bits, False)
    build(ROW1, 0, [1] * bits, True)
    parts = [phased(wave[0, b], wave[1, b], diag[0:1, :] * levels[b]) for b in range(blocks)]
    parts = mix_blocks(parts, *pair(0, 2))
    for b in range(blocks):
        work[b, 0], work[b, 1] = parts[b]

    @pl.loop(0, blocks // GROUP)
    def _(i):
        @pl.loop(i * GROUP, i * GROUP + GROUP)
        def _(b):
            xr, xi = right(LANE1, work[b, 0], work[b, 1])
            send1[b, 0], send1[b, 1] = left(ROW1, xr, xi)

        swap(0, i)

    if EARLY:
        spread(flip, tab3, tsend.at[1], trecv.at[1])

    build(DEV1, 0, device_groups, True)
    build(LANE2, 1, [0] * bits, True)
    build(ROW2, 1, [1] * bits, True)
    build(DEV2, 1, device_groups, True)
    build(DEV3, 2, device_groups, True)
    build(ROW3, 2, [1] * bits, False)
    build(LANE3, 2, [0] * bits, False)

    landed(tab2, trecv.at[0])

    @pl.loop(0, blocks // GROUP)
    def _(i):
        arrived(0, i, rsem)

        @pl.loop(i * GROUP, i * GROUP + GROUP)
        def _(b):
            xr, xi = left(DEV1, land1[b, 0, :n, :], land1[b, 1, :n, :])
            xr, xi = phased(xr, xi, diag[1:2, :] * tab2[b, :n, :])
            send2[b, 0], send2[b, 1] = turned(LANE2, xr, xi)

        swap(1, i)

    if not EARLY:
        spread(flip, tab3, tsend.at[1], trecv.at[1])

    @pl.loop(0, blocks // GROUP)
    def _(i):
        arrived(1, i, rsem)

        @pl.loop(i * GROUP, i * GROUP + GROUP)
        def _(b):
            xr, xi = left(ROW2, land2[b, 0, :n, :], land2[b, 1, :n, :])
            work[b, 0], work[b, 1] = turned(DEV2, xr, xi)

    parts = mix_blocks([(work[b, 0], work[b, 1]) for b in range(blocks)], *pair(1, 2))
    for b in range(blocks):
        work[b, 0], work[b, 1] = parts[b]
    landed(tab3, trecv.at[1])
    lane = lax.broadcasted_iota(jnp.int32, (1, n), 1)
    own = jnp.sum(jnp.where(lane == me, diag[2:3, :], 0.0), axis=1, keepdims=True)

    @pl.loop(0, blocks // GROUP)
    def _(i):
        @pl.loop(i * GROUP, i * GROUP + GROUP)
        def _(b):
            xr, xi = phased(work[b, 0], work[b, 1], own * tab3[b, :n, :])
            xr, xi = left(DEV3, xr, xi)
            send3[b, 0], send3[b, 1] = right(ROW3, xr, xi)

        swap(2, i)

    @pl.loop(0, blocks // GROUP)
    def _(i):
        arrived(2, i, rsem)

        @pl.loop(i * GROUP, i * GROUP + GROUP)
        def _(b):
            work[b, 0], work[b, 1] = right(LANE3, land3[b, 0, :n, :].T, land3[b, 1, :n, :].T)

    parts = mix_blocks([(work[b, 0], work[b, 1]) for b in range(blocks)], *pair(2, 2))
    for b in range(blocks):
        out[0, b], out[1, b] = parts[b]

    @pl.loop(0, blocks // GROUP)
    def _(i):
        for k in range(3):
            arrived(k, i, ssem)

    landed(tab2, tsend.at[0])
    landed(tab3, tsend.at[1])


def solution(mesh):
    nqa, nqb = mesh.shape["qa"], mesh.shape["qb"]

    def shards(wave_parts, level_table, diagonal_angles, turn_angles):
        _, blocks, rows, lanes = wave_parts.shape
        state = pltpu.VMEM((blocks, 2, rows, lanes), F32)
        landing = pltpu.VMEM((blocks, 2, rows + PAD, lanes), F32)
        vmem = pl.BlockSpec(memory_space=pltpu.VMEM)
        return pl.pallas_call(
            functools.partial(body, nqa, nqb),
            out_shape=jax.ShapeDtypeStruct(wave_parts.shape, F32),
            in_specs=[vmem] * 4,
            out_specs=vmem,
            scratch_shapes=[
                pltpu.VMEM((9, 2, 2 * rows, 2 * lanes), BF16),
                state,
                state,
                state,
                landing,
                landing,
                landing,
                pltpu.VMEM((blocks, rows, lanes), F32),
                pltpu.VMEM((blocks, rows + PAD, lanes), F32),
                pltpu.VMEM((blocks, rows + PAD, lanes), F32),
                state,
                pltpu.SemaphoreType.DMA((3, blocks // GROUP)),
                pltpu.SemaphoreType.DMA((3, blocks // GROUP)),
                pltpu.SemaphoreType.DMA((2,)),
                pltpu.SemaphoreType.DMA((2,)),
            ],
            name="layers",
            compiler_params=pltpu.CompilerParams(collective_id=0, has_side_effects=True),
        )(wave_parts, level_table, diagonal_angles, turn_angles)

    return jax.shard_map(
        shards,
        mesh=mesh,
        in_specs=(
            P("trial", ("qa", "qb"), None, None),
            P(("trial", "qa", "qb"), None, None),
            P("trial", None),
            P("trial", None),
        ),
        out_specs=P("trial", ("qa", "qb"), None, None),
        check_vma=False,
    )
```

```python
import functools

import jax
import jax.numpy as jnp
from jax import lax
from jax.experimental import pallas as pl
from jax.experimental.pallas import tpu as pltpu
from jax.sharding import PartitionSpec as P

MESH = pl.DeviceIdType.MESH
F32 = jnp.float32
BF16 = jnp.bfloat16
PAD = 8


def split(x):
    high = x.astype(BF16)
    return high, (x - high.astype(F32)).astype(BF16)


def dot3(a, b, dims=((1,), (0,))):
    def one(x, y):
        return lax.dot_general(x, y, (dims, ((), ())), preferred_element_type=F32)

    (ah, al), (bh, bl) = a, b
    return one(ah, bh) + (one(ah, bl) + one(al, bh))


def sincos(x):
    turns = jnp.floor(x * 0.6366197723675814 + 0.5)
    y = (x - turns * 1.5707855224609375) - turns * 1.0804334124e-05
    z = y * y
    s = y + y * z * (-1.6666654611e-1 + z * (8.3321608736e-3 + z * -1.9515295891e-4))
    c = 1.0 - 0.5 * z + z * z * (4.166664568298827e-2 + z * (-1.388731625493765e-3 + z * 2.443315711809948e-5))
    quarter = turns - 4.0 * jnp.floor(turns * 0.25)
    odd = (quarter == 1.0) | (quarter == 3.0)
    sin = jnp.where(odd, c, s)
    cos = jnp.where(odd, s, c)
    sin = jnp.where(quarter >= 2.0, -sin, sin)
    cos = jnp.where((quarter == 1.0) | (quarter == 2.0), -cos, cos)
    return sin, cos


def rotated(xr, xi, s, c):
    return xr * c + xi * s, xi * c - xr * s


def phased(xr, xi, turn):
    return rotated(xr, xi, *sincos(turn))


def rotation(count, pairs):
    apart = lax.broadcasted_iota(jnp.int32, (count, count), 0) ^ lax.broadcasted_iota(jnp.int32, (count, count), 1)
    size = None
    ones = None
    for place, (c, s) in enumerate(pairs):
        bit = (apart >> place) & 1
        factor = jnp.where(bit == 1, s, c)
        size = factor if size is None else size * factor
        ones = bit if ones is None else ones + bit
    ones = ones & 3
    real = jnp.where(ones == 0, size, jnp.where(ones == 2, -size, 0.0))
    imag = jnp.where(ones == 1, -size, jnp.where(ones == 3, size, 0.0))
    return real, imag


def mix_blocks(parts, c, s):
    step = 1
    while step < len(parts):
        mixed = list(parts)
        for k in range(len(parts)):
            if not k & step:
                (ur, ui), (vr, vi) = parts[k], parts[k | step]
                mixed[k] = (c * ur + s * vi, c * ui - s * vr)
                mixed[k | step] = (c * vr + s * ui, c * vi - s * ur)
        parts = mixed
        step *= 2
    return parts


def body(
    nqa,
    nqb,
    wave,
    levels,
    diag,
    turns,
    out,
    mats,
    send1,
    send2,
    send3,
    land1,
    land2,
    land3,
    flip,
    tab2,
    tab3,
    work,
    phase,
    ssem,
    rsem,
    tsend,
    trecv,
):
    n = nqa * nqb
    blocks = wave.shape[1]
    qa = lax.axis_index("qa")
    qb = lax.axis_index("qb")
    me = qa * nqb + qb
    near = list(range(1, nqb))
    near.sort(key=lambda d: -min(d, nqb - d))

    def peers(visit):
        @pl.loop(1, nqa)
        def _(da):
            for dz in near + [0]:
                visit(lax.rem(qa + da, nqa), lax.rem(qb + dz, nqb))

        for dz in near:
            visit(qa, lax.rem(qb + dz, nqb))

    bar = pltpu.get_barrier_semaphore()
    peers(lambda a, z: pl.semaphore_signal(bar, inc=1, device_id={"qa": a, "qb": z}, device_id_type=MESH))

    def spread(src, dst, ssem, rsem):
        def visit(a, z):
            pltpu.make_async_remote_copy(
                src_ref=src.at[..., pl.ds(a * nqb + z, 1), :],
                dst_ref=dst.at[..., pl.ds(me, 1), :],
                send_sem=ssem,
                recv_sem=rsem,
                device_id={"qa": a, "qb": z},
                device_id_type=MESH,
            ).start()

        peers(visit)
        pltpu.make_async_remote_copy(
            src_ref=src.at[..., pl.ds(0, 1), :],
            dst_ref=dst.at[..., pl.ds(n, 1), :],
            send_sem=ssem,
            recv_sem=rsem,
            device_id={"qa": qa, "qb": lax.rem(qb + 1, nqb)},
            device_id_type=MESH,
        ).start()
        dst[..., pl.ds(me, 1), :] = src[..., pl.ds(me, 1), :]

    def swap(k):
        spread((send1, send2, send3)[k], (land1, land2, land3)[k], ssem.at[k], rsem.at[k])

    def arrived(k, sems):
        landed((land1, land2, land3)[k], sems.at[k])

    def landed(dst, rsem):
        whole = dst.at[..., pl.ds(0, n), :]
        pltpu.make_async_copy(whole, whole, rsem).wait()

    turn_sin, turn_cos = sincos(turns[...])

    def pair(layer, group):
        return turn_cos[layer : layer + 1, group : group + 1], turn_sin[layer : layer + 1, group : group + 1]

    bits = n.bit_length() - 1
    low = nqb.bit_length() - 1

    def build(slot, layer, groups, left):
        real, imag = rotation(n, [pair(layer, g) for g in groups])
        if left:
            whole = jnp.concatenate(
                [jnp.concatenate([real, -imag], axis=1), jnp.concatenate([imag, real], axis=1)], axis=0
            )
        else:
            whole = jnp.concatenate(
                [jnp.concatenate([real, imag], axis=1), jnp.concatenate([-imag, real], axis=1)], axis=0
            )
        high, rest = split(whole)
        mats[slot, 0] = high
        mats[slot, 1] = rest

    device_groups = [3] * low + [2] * (bits - low)
    LANE1, ROW1, DEV1, LANE2, ROW2, DEV2, DEV3, ROW3, LANE3 = range(9)

    def mat(slot):
        return mats[slot, 0], mats[slot, 1]

    def left(slot, xr, xi):
        both = dot3(mat(slot), split(jnp.concatenate([xr, xi], axis=0)))
        return both[:n], both[n:]

    def right(slot, xr, xi):
        both = dot3(split(jnp.concatenate([xr, xi], axis=1)), mat(slot))
        return both[:, :n], both[:, n:]

    def turned(slot, xr, xi):
        both = dot3(mat(slot), split(jnp.concatenate([xr, xi], axis=1)), ((1,), (1,)))
        return both[:n], both[n:]

    for b in range(blocks):
        flip[b] = levels[b].T
    build(LANE1, 0, [0] * bits, False)
    build(ROW1, 0, [1] * bits, True)
    parts = [phased(wave[0, b], wave[1, b], diag[0:1, :] * levels[b]) for b in range(blocks)]
    parts = mix_blocks(parts, *pair(0, 2))
    for b in range(blocks):
        work[b, 0], work[b, 1] = parts[b]
    pl.semaphore_wait(bar, n - 1)
    spread(levels, tab2, tsend.at[0], trecv.at[0])
    for b in range(blocks):
        xr, xi = right(LANE1, work[b, 0], work[b, 1])
        send1[b, 0], send1[b, 1] = left(ROW1, xr, xi)
    swap(0)

    spread(flip, tab3, tsend.at[1], trecv.at[1])

    build(DEV1, 0, device_groups, True)
    build(LANE2, 1, [0] * bits, True)
    build(ROW2, 1, [1] * bits, True)
    build(DEV2, 1, device_groups, True)
    build(DEV3, 2, device_groups, True)
    build(ROW3, 2, [1] * bits, False)
    build(LANE3, 2, [0] * bits, False)

    landed(tab2, trecv.at[0])
    for b in range(blocks):
        phase[b, 0], phase[b, 1] = sincos(diag[1:2, :] * tab2[b, :n, :])
    arrived(0, rsem)
    for b in range(blocks):
        xr, xi = left(DEV1, land1[b, 0, :n, :], land1[b, 1, :n, :])
        xr, xi = rotated(xr, xi, phase[b, 0], phase[b, 1])
        send2[b, 0], send2[b, 1] = turned(LANE2, xr, xi)
    swap(1)

    lane = lax.broadcasted_iota(jnp.int32, (1, n), 1)
    own = jnp.sum(jnp.where(lane == me, diag[2:3, :], 0.0), axis=1, keepdims=True)
    landed(tab3, trecv.at[1])
    for b in range(blocks):
        phase[b, 0], phase[b, 1] = sincos(own * tab3[b, :n, :])
    arrived(1, rsem)
    for b in range(blocks):
        xr, xi = left(ROW2, land2[b, 0, :n, :], land2[b, 1, :n, :])
        work[b, 0], work[b, 1] = turned(DEV2, xr, xi)
    parts = mix_blocks([(work[b, 0], work[b, 1]) for b in range(blocks)], *pair(1, 2))
    for b in range(blocks):
        xr, xi = rotated(*parts[b], phase[b, 0], phase[b, 1])
        work[b, 0], work[b, 1] = left(DEV3, xr, xi)
    for b in range(blocks):
        send3[b, 0], send3[b, 1] = right(ROW3, work[b, 0], work[b, 1])
    swap(2)

    arrived(2, rsem)
    for b in range(blocks):
        work[b, 0], work[b, 1] = right(LANE3, land3[b, 0, :n, :].T, land3[b, 1, :n, :].T)
    parts = mix_blocks([(work[b, 0], work[b, 1]) for b in range(blocks)], *pair(2, 2))
    for b in range(blocks):
        out[0, b], out[1, b] = parts[b]

    for k in range(3):
        arrived(k, ssem)

    landed(tab2, tsend.at[0])
    landed(tab3, tsend.at[1])


def solution(mesh):
    nqa, nqb = mesh.shape["qa"], mesh.shape["qb"]

    def shards(wave_parts, level_table, diagonal_angles, turn_angles):
        _, blocks, rows, lanes = wave_parts.shape
        state = pltpu.VMEM((blocks, 2, rows, lanes), F32)
        landing = pltpu.VMEM((blocks, 2, rows + PAD, lanes), F32)
        vmem = pl.BlockSpec(memory_space=pltpu.VMEM)
        return pl.pallas_call(
            functools.partial(body, nqa, nqb),
            out_shape=jax.ShapeDtypeStruct(wave_parts.shape, F32),
            in_specs=[vmem] * 4,
            out_specs=vmem,
            scratch_shapes=[
                pltpu.VMEM((9, 2, 2 * rows, 2 * lanes), BF16),
                state,
                state,
                state,
                landing,
                landing,
                landing,
                pltpu.VMEM((blocks, rows, lanes), F32),
                pltpu.VMEM((blocks, rows + PAD, lanes), F32),
                pltpu.VMEM((blocks, rows + PAD, lanes), F32),
                state,
                state,
                pltpu.SemaphoreType.DMA((3,)),
                pltpu.SemaphoreType.DMA((3,)),
                pltpu.SemaphoreType.DMA((2,)),
                pltpu.SemaphoreType.DMA((2,)),
            ],
            name="layers",
            compiler_params=pltpu.CompilerParams(collective_id=0, has_side_effects=True),
        )(wave_parts, level_table, diagonal_angles, turn_angles)

    return jax.shard_map(
        shards,
        mesh=mesh,
        in_specs=(
            P("trial", ("qa", "qb"), None, None),
            P(("trial", "qa", "qb"), None, None),
            P("trial", None),
            P("trial", None),
        ),
        out_specs=P("trial", ("qa", "qb"), None, None),
        check_vma=False,
    )
```
